256 devices in a mesh: member: 2 (over y), lat: 128 (over z, x, core).
Axes of the slice: x: 4, y: 2, z: 16, core: 2. Of those that a mesh axis runs over, the one named last changes fastest.
The devices are a block of a 4x16x16 slice.
Arguments:
- tracers: float32 [60, 4, 512, 1440], P('member', None, 'lat'), parts along dimension 0, may hold values from -6 to 6
- currents: float32 [4, 4, 512, 1440], P('member', None, 'lat'), parts along dimension 0, may hold values from -0.4 to 0.4
- column_levels: int32 [1024, 1440], P(('member', 'lat')), parts along dimension 0, may hold values from 0 to 4
Outputs:
- advected: float32 [60, 4, 512, 1440], P('member', None, 'lat'), parts along dimension 0
The draws below stay inside these ranges and needn't reach their ends.
There are 2 independent parts, one for each index of `member`. The reference program is written for one: setup_inputs(seed, part) draws one part's arguments, and reference() takes and returns one part's arrays. A program takes and returns all parts, laid end to end along the dimension named above; each array names one. Nothing has to cross between parts.
All inputs are finite; a program needn't handle non-finite values.
Results may differ from the reference program's by a relative error of at most 0.00002.
Values sent between devices are 32-bit elements; how exact they have to be, the bound alone decides.
No kernel may reach another device: no remote copies, remote signals or barrier semaphores. Data moves between devices by JAX's collectives and lax.ppermute only.
A program may use at most 64 MiB of HBM per device.

```python
import jax
import jax.numpy as jnp

TRACERS = 30
LEVELS = 4
NLON = 1440
NLAT = 512


def place_ends(values, own_key, least, top_value):
    longest = values.shape.index(max(values.shape))
    spots = []
    for shift in (0, 1):
        where = [jax.random.randint(jax.random.fold_in(own_key, axis), (), 0, length) for axis, length in enumerate(values.shape)]
        where[longest] = (where[longest] + shift) % values.shape[longest]
        spots.append(tuple(where))
    return values.at[spots[0]].set(least).at[spots[1]].set(top_value)


def shard_levels(rng, shape, shards, least, high):
    level, own = 1.0, jax.random.fold_in(rng, 6)
    for position, parts in shards:
        steps = jnp.exp(jax.random.uniform(jax.random.fold_in(own, position), (parts,), jnp.float32, least / len(shards), high / len(shards)))
        level = level * jnp.repeat(steps, shape[position] // parts).reshape([-1 if axis == position else 1 for axis in range(len(shape))])
    return level


def scatter_about(rng, dims, spread, limit, pieces=(), kind=jnp.bfloat16):
    gain = shard_levels(rng, dims, pieces, -0.22, 0.18) if pieces else 1.0
    result = jax.random.normal(rng, dims, jnp.float32) * spread * gain
    return jnp.minimum(jnp.maximum(result, -limit), limit).astype(kind)


def setup_inputs(seed: int = 0, part: int = 0) -> dict:
    splits = jax.random.split(jax.random.key(seed), 4)
    part_splits = jax.random.split(jax.random.fold_in(splits[3], part), 4)
    tracers = scatter_about(part_splits[0], (TRACERS, LEVELS, NLAT, NLON), 1.0, 6.0, ((2, 128),), jnp.float32)
    currents = jnp.clip(jax.random.uniform(part_splits[1], (2, LEVELS, NLAT, NLON), jnp.float32, -0.4, 0.4) * shard_levels(part_splits[1], (2, LEVELS, NLAT, NLON), ((2, 128),), -0.4, 0.0), -0.4, 0.4)
    column_levels = place_ends(jax.random.randint(part_splits[2], (NLAT, NLON), 0, LEVELS + 1), jax.random.fold_in(part_splits[2], 1), 0, LEVELS).astype(jnp.int32)
    return {"tracers": tracers, "currents": currents, "column_levels": column_levels}


def face_flux(courant, before, left, right, after):
    central = courant * (7.0 * (left + right) - (before + after)) / 12.0
    upwind = jnp.abs(courant) * (3.0 * (right - left) - (after - before)) / 12.0
    return central - upwind


def advect_section(padded, east_pad, north_pad, wet_pad):
    rows = padded.shape[-2] - 4
    field = padded[..., 2:-2, :]
    east = east_pad[:, 1:-1]
    wet_rows = wet_pad[:, 1:-1]
    east_face = 0.5 * (east + jnp.roll(east, -1, -1))
    east_open = wet_rows * jnp.roll(wet_rows, -1, -1)
    east_flux = east_open * face_flux(east_face, jnp.roll(field, 1, -1), field, jnp.roll(field, -1, -1), jnp.roll(field, -2, -1))
    east_div = east_flux - jnp.roll(east_flux, 1, -1)
    north_face = 0.5 * (north_pad[:, :-1] + north_pad[:, 1:])
    north_open = wet_pad[:, :-1] * wet_pad[:, 1:]
    north_flux = north_open * face_flux(north_face, padded[..., 0:rows + 1, :], padded[..., 1:rows + 2, :], padded[..., 2:rows + 3, :], padded[..., 3:rows + 4, :])
    north_div = north_flux[..., 1:, :] - north_flux[..., :-1, :]
    return field - east_div - north_div


def extend(field, width, factor):
    south = jnp.zeros(field.shape[:-2] + (width, field.shape[-1]), jnp.float32)
    north = factor * jnp.flip(field[..., field.shape[-2] - width:, :], axis=(-2, -1))
    return jnp.concatenate([south, field, north], axis=-2)


def reference(tracers, currents, column_levels):
    levels = jnp.arange(tracers.shape[1], dtype=jnp.int32)
    wet = (levels[:, None, None] < column_levels[None]).astype(jnp.float32)
    east_pad = extend(currents[0], 1, -1.0)
    north_pad = extend(currents[1], 1, -1.0)
    wet_pad = extend(wet, 1, 1.0)
    start = tracers * wet
    first = advect_section(extend(start, 2, 1.0), east_pad, north_pad, wet_pad) * wet
    second = advect_section(extend(first, 2, 1.0), east_pad, north_pad, wet_pad)
    return 0.5 * (start + second) * wet
```

```python
import functools

import jax
import jax.numpy as jnp
from jax import lax
from jax.experimental import pallas as pl
from jax.experimental.pallas import tpu as pltpu
from jax.sharding import PartitionSpec as P


LANES = 128
SMALL = 24
CHUNKS = (8, 16, 6)


def lane_index():
    return lax.broadcasted_iota(jnp.int32, (8, LANES), 1)


def spread(ref, row):
    return jnp.broadcast_to(ref[pl.ds(row, 1), :], (8, LANES))


def wrap_tile(raw, first, rem):
    lane = lane_index()
    wrapped = jnp.where(
        lane < LANES - rem, pltpu.roll(first, rem, 1), pltpu.roll(raw, LANES - rem, 1)
    )
    return jnp.where(lane < rem, raw, wrapped)


def shifted(tiles, t, by):
    lane = lane_index()
    count = len(tiles)
    if by > 0:
        here, there = tiles[t], tiles[(t + 1) % count]
        keep = lane < LANES - by
    else:
        here, there = tiles[t], tiles[(t - 1) % count]
        keep = lane >= -by
    amount = (-by) % LANES
    return jnp.where(keep, pltpu.roll(here, amount, 1), pltpu.roll(there, amount, 1))


def mirrored(tiles, rem):
    lane = lane_index()
    index = (rem - 1 - lane) % LANES
    turned = [jnp.take_along_axis(tile, index, axis=1, mode="promise_in_bounds") for tile in tiles]
    last = len(tiles) - 1
    out = [jnp.where(lane < rem, turned[last - t], turned[last - 1 - t]) for t in range(last)]
    out.append(wrap_tile(turned[0], out[0], rem))
    return out


def natural_tile(ref, where, t, lon):
    full, rem = divmod(lon, LANES)
    if t < full:
        return ref[(*where, slice(None), pl.ds(t * LANES, LANES))]
    tail = ref[(*where, slice(None), pl.ds(full * LANES, rem))]
    head = ref[(*where, slice(None), pl.ds(0, LANES))][:, : LANES - 2 * rem]
    return jnp.concatenate([tail, head, tail], axis=1)


def stage_currents(currents, levels, held, lon):
    tiles = lon // LANES + 1
    for t in range(tiles):
        for c in range(2):
            for half in range(2):
                pair = [natural_tile(currents, (c, 2 * half + k), t, lon) for k in range(2)]
                held[pl.ds((t * 5 + 2 * c + half) * 8, 8), :] = jnp.concatenate(pair, axis=0)
        column = natural_tile(levels, (), t, lon).astype(jnp.float32)
        held[pl.ds((t * 5 + 4) * 8, 8), :] = jnp.concatenate([column, column], axis=0)


def own_row(held, t, c, row):
    return held[pl.ds((t * 5 + 2 * c) * 8 + row, 4, stride=4), :]


def edge_rows(held, out, base, north, lon):
    u0, v0 = jnp.where(north, 2, 0), jnp.where(north, 1, 0)
    for t in range(lon // LANES + 1):
        u = [own_row(held, t, 0, u0 + k) for k in range(2)]
        v = [own_row(held, t, 1, v0 + k) for k in range(3)]
        column = held[pl.ds((t * 5 + 4) * 8, 4), :]
        start = base + t * SMALL
        out[pl.ds(start, 8), :] = jnp.concatenate(u, axis=0)
        out[pl.ds(start + 8, 8), :] = jnp.concatenate(v[:2], axis=0)
        out[pl.ds(start + 16, 8), :] = jnp.concatenate([v[2], column], axis=0)


def pack_kernel(offset, n, lon, small, *refs):
    if small:
        x_hbm, currents, levels, out, near_small, x, held, sem = refs
    else:
        x_hbm, out, x, sem = refs
    full, rem = divmod(lon, LANES)
    copy = pltpu.make_async_copy(x_hbm.at[pl.ds(offset, n)], x, sem)
    copy.start()
    if small:
        odd = lax.axis_index("lat") % 2 == 1
        stage_currents(currents, levels, held, lon)
        edge_rows(held, out, (16 * full + 4) * n, odd, lon)
        edge_rows(held, near_small, 0, jnp.logical_not(odd), lon)
    copy.wait()

    def pair(g, carry):
        tails = []
        for k in range(2):
            for half in range(2):
                for t in range(full):
                    rows = [x[2 * g + k, 2 * half + s, :, pl.ds(t * LANES, LANES)] for s in range(2)]
                    start = pl.multiple_of((t * n + 2 * g + k) * 16 + 8 * half, 8)
                    out[pl.ds(start, 8), :] = jnp.concatenate(rows, axis=0)
            tail = [x[2 * g + k, level, :, pl.ds(full * LANES, rem)] for level in range(4)]
            tails.append(jnp.concatenate(tail, axis=1))
        start = pl.multiple_of(16 * full * n + 8 * g, 8)
        out[pl.ds(start, 8), :] = jnp.concatenate(tails, axis=0)
        return carry

    lax.fori_loop(0, n // 2, pair, 0)


def coefficient_kernel(n, lon, currents, levels, near, far, k1, k2, held, u, v, w):
    full, rem = divmod(lon, LANES)
    tiles = full + 1
    far_base = (16 * full + 4) * n
    place = lax.axis_index("lat")
    odd = place % 2 == 1
    level = (lax.broadcasted_iota(jnp.int32, (8, LANES), 0) % 4).astype(jnp.float32)
    stage_currents(currents, levels, held, lon)

    def put(dst, row, t, value):
        dst[pl.ds((row * tiles + t) * 8, 8), :] = value

    def get(src, row):
        return [src[pl.ds((row * tiles + t) * 8, 8), :] for t in range(tiles)]

    def twice(value):
        return jnp.concatenate([value, value], axis=0)

    for t in range(tiles):
        for row in range(4):
            put(u, 2 + row, t, twice(own_row(held, t, 0, row)))
            put(v, 3 + row, t, twice(own_row(held, t, 1, row)))
            column = spread(held, (t * 5 + 4) * 8 + row)
            put(w, 4 + row, t, (level < column).astype(jnp.float32))
        sides = ((0, 0, 0, True), (6, 7, 8, False))
        for u_row, v_row, w_row, is_low in sides:
            take_near = odd if is_low else jnp.logical_not(odd)

            def pick(start, size):
                a = near[pl.ds(t * SMALL + start, size), :]
                b = far[pl.ds(far_base + t * SMALL + start, size), :]
                return jnp.where(take_near, a, b)

            for k in range(2):
                put(u, u_row + k, t, twice(pick(4 * k, 4)))
            for k in range(3):
                put(v, v_row + k, t, twice(pick(8 + 4 * k, 4)))
            for k in range(4):
                put(w, w_row + k, t, (level < jnp.broadcast_to(pick(20 + k, 1), level.shape)).astype(jnp.float32))

    @pl.when(place == lax.axis_size("lat") - 1)
    def _():
        for dst, first, count, sign in ((u, 6, 2, -1.0), (v, 7, 3, -1.0), (w, 8, 4, 1.0)):
            for k in range(count):
                for t, value in enumerate(mirrored(get(dst, first - 1 - k), rem)):
                    put(dst, first + k, t, sign * value)

    def parts(face):
        return jnp.maximum(face, 0.0) * (1.0 / 6.0), jnp.minimum(face, 0.0) * (1.0 / 6.0)

    def north_faces(row):
        wa, wb, va, vb = get(w, row + 4), get(w, row + 5), get(v, row + 3), get(v, row + 4)
        return [parts(wa[t] * wb[t] * (0.5 * (va[t] + vb[t]))) for t in range(tiles)]

    south = north_faces(-3)
    for row in range(-2, 6):
        north = north_faces(row)
        ur = get(u, row + 2)
        wr = {d: get(w, row + 4 + d) for d in (-2, -1, 0, 1, 2)}
        we = {d: [shifted(wr[0], t, d) for t in range(tiles)] for d in (-2, -1, 1, 2)}
        east = [parts(wr[0][t] * we[1][t] * (0.5 * (ur[t] + shifted(ur, t, 1)))) for t in range(tiles)]
        west_p = [shifted([e[0] for e in east], t, -1) for t in range(tiles)]
        west_m = [shifted([e[1] for e in east], t, -1) for t in range(tiles)]
        for t in range(tiles):
            (p, m), (q, s), (qs, ss) = east[t], north[t], south[t]
            pw, mw = west_p[t], west_m[t]
            plain = [
                -pw,
                p + 5.0 * pw + 2.0 * mw,
                -(2.0 * p + 5.0 * m + mw),
                m,
                1.0 - (5.0 * p + 2.0 * m) + (2.0 * pw + 5.0 * mw) - (5.0 * q + 2.0 * s) + (2.0 * qs + 5.0 * ss),
                -qs,
                q + 5.0 * qs + 2.0 * ss,
                -(2.0 * q + 5.0 * s + ss),
                s,
            ]
            source = [we[-2][t], we[-1][t], we[1][t], we[2][t], wr[0][t], wr[-2][t], wr[-1][t], wr[1][t], wr[2][t]]
            here = wr[0][t]
            for k in range(9):
                k1[pl.ds((((row + 2) * tiles + t) * 9 + k) * 8, 8), :] = plain[k] * source[k] * here
            if 0 <= row < 4:
                half = 0.5 * here
                for k in range(9):
                    k2[pl.ds(((row * tiles + t) * 10 + k) * 8, 8), :] = plain[k] * half
                k2[pl.ds(((row * tiles + t) * 10 + 9) * 8, 8), :] = half * here
        south = north


def stencil(coefficient, lon_row, rows, t):
    values = [shifted(lon_row, t, d) for d in (-2, -1, 1, 2)] + [lon_row[t]] + rows
    total = coefficient(0) * values[0]
    for k in range(1, 9):
        total = total + coefficient(k) * values[k]
    return total


def advect_kernel(n, lon, own, near, far, k1, k2, *refs):
    out, f, first, turned = refs[-4:]
    full, rem = divmod(lon, LANES)
    tiles = full + 1
    row_size = tiles * 8
    g = pl.program_id(0)
    place = lax.axis_index("lat")
    odd = place % 2 == 1
    sub = lax.broadcasted_iota(jnp.int32, (8, LANES), 0)

    near_base = jnp.where(odd, 0, 8) * row_size
    far_base = jnp.where(odd, 8, 0) * row_size
    for source, base in ((near, near_base), (own, 4 * row_size), (far, far_base)):
        for r in range(4):
            for t in range(full):
                value = source[pl.ds((t * n + 2 * g) * 16 + r, 8, stride=4), :]
                f[pl.ds(pl.multiple_of(base + (r * tiles + t) * 8, 8), 8), :] = value
                if t == 0:
                    start = value
            tail = 16 * full * n + 8 * g
            a = spread(source, tail + r)
            b = spread(source, tail + 4 + r)
            both = jnp.where(sub < 4, a, b)
            raw = both
            for level in range(1, 4):
                raw = jnp.where(sub % 4 == level, pltpu.roll(both, LANES - rem * level, 1), raw)
            f[pl.ds(pl.multiple_of(base + (r * tiles + full) * 8, 8), 8), :] = wrap_tile(raw, start, rem)

    def row_of(ref, row):
        return [ref[pl.ds((row * tiles + t) * 8, 8), :] for t in range(tiles)]

    @pl.when(place == lax.axis_size("lat") - 1)
    def _():
        for k in range(4):
            for t, value in enumerate(mirrored(row_of(f, 7 - k), rem)):
                f[pl.ds(((8 + k) * tiles + t) * 8, 8), :] = value

    for row in range(8):
        lon_row = row_of(f, row + 2)
        for t in range(tiles):
            rows = [f[pl.ds(((row + 2 + d) * tiles + t) * 8, 8), :] for d in (-2, -1, 1, 2)]
            base = (row * tiles + t) * 9
            value = stencil(lambda k: k1[pl.ds((base + k) * 8, 8), :], lon_row, rows, t)
            first[pl.ds((row * tiles + t) * 8, 8), :] = value

    for row in range(4):
        lon_row = row_of(first, row + 2)
        for t in range(tiles):
            rows = [first[pl.ds(((row + 2 + d) * tiles + t) * 8, 8), :] for d in (-2, -1, 1, 2)]
            base = (row * tiles + t) * 10
            value = stencil(lambda k: k2[pl.ds((base + k) * 8, 8), :], lon_row, rows, t)
            value = value + k2[pl.ds((base + 9) * 8, 8), :] * f[pl.ds(((row + 4) * tiles + t) * 8, 8), :]
            turned[pl.ds(t * 32 + row, 8, stride=4), :] = value

    for k in range(2):
        for level in range(4):
            for t in range(tiles):
                value = turned[pl.ds(t * 32 + (4 * k + level) * 4, 4), :]
                if t < full:
                    out[k, level, :, pl.ds(t * LANES, LANES)] = value
                else:
                    out[k, level, :, pl.ds(full * LANES, rem)] = value[:, :rem]


def vmem():
    return pl.BlockSpec(memory_space=pltpu.VMEM)


def shards(tracers, currents, column_levels):
    count = lax.axis_size("lat")
    total, levels, rows, lon = tracers.shape
    full, rem = divmod(lon, LANES)
    tiles = full + 1
    assert levels == 4 and rows == 4 and 4 * rem == LANES and count % 2 == 0 and sum(CHUNKS) == total
    near_pairs = [(i, i ^ 1) for i in range(count)]
    far_pairs = [pair for i in range(1, count - 1, 2) for pair in ((i, i + 1), (i + 1, i))]
    f32 = jnp.float32
    offsets = [sum(CHUNKS[:i]) for i in range(len(CHUNKS))]

    packed, near_small = [], None
    for i, (offset, n) in enumerate(zip(offsets, CHUNKS)):
        small = i == 0
        size = (16 * full + 4) * n
        shape = [jax.ShapeDtypeStruct((size + (SMALL * tiles if small else 0), LANES), f32)]
        scratch = [pltpu.VMEM((n, levels, rows, lon), f32), pltpu.SemaphoreType.DMA]
        if small:
            shape.append(jax.ShapeDtypeStruct((SMALL * tiles, LANES), f32))
            scratch.insert(1, pltpu.VMEM((tiles * 40, LANES), f32))
        result = pl.pallas_call(
            functools.partial(pack_kernel, offset, n, lon, small),
            out_shape=shape,
            in_specs=[pl.BlockSpec(memory_space=pl.ANY)] + [vmem()] * (2 if small else 0),
            out_specs=[vmem() for _ in shape],
            scratch_shapes=scratch,
            cost_estimate=pl.CostEstimate(flops=1000000 * n, bytes_accessed=n * 184320, transcendentals=0),
            compiler_params=pltpu.CompilerParams(vmem_limit_bytes=16 * 2**20),
        )(tracers, *((currents, column_levels) if small else ()))
        packed.append(result[0])
        if small:
            near_small = result[1]
    far = []
    for i in range(len(CHUNKS)):
        far.append(lax.ppermute(packed[i], "lat", far_pairs))
    small_received = lax.ppermute(near_small, "lat", near_pairs)
    near = []
    for i in range(len(CHUNKS)):
        near.append(lax.ppermute(packed[i], "lat", near_pairs))
    k1, k2 = pl.pallas_call(
        functools.partial(coefficient_kernel, CHUNKS[0], lon),
        out_shape=[
            jax.ShapeDtypeStruct((8 * tiles * 9 * 8, LANES), f32),
            jax.ShapeDtypeStruct((4 * tiles * 10 * 8, LANES), f32),
        ],
        in_specs=[vmem()] * 4,
        out_specs=[vmem()] * 2,
        scratch_shapes=[
            pltpu.VMEM((tiles * 40, LANES), f32),
            pltpu.VMEM((8 * tiles * 8, LANES), f32),
            pltpu.VMEM((10 * tiles * 8, LANES), f32),
            pltpu.VMEM((12 * tiles * 8, LANES), f32),
        ],
        cost_estimate=pl.CostEstimate(flops=8000000, bytes_accessed=6000000, transcendentals=0),
        compiler_params=pltpu.CompilerParams(vmem_limit_bytes=20 * 2**20),
        name="coefficients",
    )(currents, column_levels, small_received, far[0])
    out = None
    for i, (offset, n) in enumerate(zip(offsets, CHUNKS)):
        operands = [packed[i], near[i], far[i], k1, k2]
        specs = [vmem()] * 5
        aliases = {}
        if out is not None:
            aliases = {len(operands): 0}
            operands.append(out)
            specs.append(pl.BlockSpec(memory_space=pl.ANY))
        out = pl.pallas_call(
            functools.partial(advect_kernel, n, lon),
            out_shape=jax.ShapeDtypeStruct(tracers.shape, f32),
            grid=(n // 2,),
            in_specs=specs,
            out_specs=pl.BlockSpec((2, levels, rows, lon), lambda g, o=offset // 2: (o + g, 0, 0, 0)),
            scratch_shapes=[
                pltpu.VMEM((12 * tiles * 8, LANES), f32),
                pltpu.VMEM((8 * tiles * 8, LANES), f32),
                pltpu.VMEM((32 * tiles, LANES), f32),
            ],
            input_output_aliases=aliases,
            cost_estimate=pl.CostEstimate(flops=3000000 * n, bytes_accessed=n * 500000, transcendentals=0),
            compiler_params=pltpu.CompilerParams(vmem_limit_bytes=24 * 2**20),
        )(*operands)
    return out


def solution(mesh):
    in_specs = (
        P("member", None, "lat", None),
        P("member", None, "lat", None),
        P(("member", "lat"), None),
    )
    out_specs = P("member", None, "lat", None)
    return jax.shard_map(shards, mesh=mesh, in_specs=in_specs, out_specs=out_specs, check_vma=False)
```

```python
import functools

import jax
import jax.numpy as jnp
from jax import lax
from jax.experimental import pallas as pl
from jax.experimental.pallas import tpu as pltpu
from jax.sharding import PartitionSpec as P


LANES = 128
SMALL = 24
CHUNKS = (12, 8, 6, 4)
OFFSETS = (0, 12, 24, 20)
GROUPS = (3, 2, 3, 2)


def lane_index():
    return lax.broadcasted_iota(jnp.int32, (8, LANES), 1)


def spread(ref, row):
    return jnp.broadcast_to(ref[pl.ds(row, 1), :], (8, LANES))


def wrap_tile(raw, first, rem):
    lane = lane_index()
    wrapped = jnp.where(
        lane < LANES - rem, pltpu.roll(first, rem, 1), pltpu.roll(raw, LANES - rem, 1)
    )
    return jnp.where(lane < rem, raw, wrapped)


def shifted(tiles, t, by):
    count = len(tiles)
    if by > 0:
        joined = jnp.where(lane_index() < by, tiles[(t + 1) % count], tiles[t])
    else:
        joined = jnp.where(lane_index() >= LANES + by, tiles[(t - 1) % count], tiles[t])
    return pltpu.roll(joined, (-by) % LANES, 1)


def mirrored(tiles, rem):
    lane = lane_index()
    index = (rem - 1 - lane) % LANES
    turned = [jnp.take_along_axis(tile, index, axis=1, mode="promise_in_bounds") for tile in tiles]
    last = len(tiles) - 1
    out = [jnp.where(lane < rem, turned[last - t], turned[last - 1 - t]) for t in range(last)]
    return [*out, turned[0]]


def natural_tile(ref, where, t, lon):
    full, rem = divmod(lon, LANES)
    if t < full:
        return ref[(*where, slice(None), pl.ds(t * LANES, LANES))]
    tail = ref[(*where, slice(None), pl.ds(full * LANES, rem))]
    head = ref[(*where, slice(None), pl.ds(0, LANES))][:, : LANES - 2 * rem]
    return jnp.concatenate([tail, head, tail], axis=1)


def stage_currents(currents, levels, held, lon):
    tiles = lon // LANES + 1
    for t in range(tiles):
        for c in range(2):
            for half in range(2):
                pair = [natural_tile(currents, (c, 2 * half + k), t, lon) for k in range(2)]
                held[pl.ds((t * 5 + 2 * c + half) * 8, 8), :] = jnp.concatenate(pair, axis=0)
        column = natural_tile(levels, (), t, lon).astype(jnp.float32)
        held[pl.ds((t * 5 + 4) * 8, 8), :] = jnp.concatenate([column, column], axis=0)


def own_row(held, t, c, row):
    return held[pl.ds((t * 5 + 2 * c) * 8 + row, 4, stride=4), :]


def edge_rows(held, out, base, north, lon):
    u0, v0 = jnp.where(north, 2, 0), jnp.where(north, 1, 0)
    for t in range(lon // LANES + 1):
        u = [own_row(held, t, 0, u0 + k) for k in range(2)]
        v = [own_row(held, t, 1, v0 + k) for k in range(3)]
        column = held[pl.ds((t * 5 + 4) * 8, 4), :]
        start = base + t * SMALL
        out[pl.ds(start, 8), :] = jnp.concatenate(u, axis=0)
        out[pl.ds(start + 8, 8), :] = jnp.concatenate(v[:2], axis=0)
        out[pl.ds(start + 16, 8), :] = jnp.concatenate([v[2], column], axis=0)


def folded_edge_rows(held, out, base, lon):
    tiles, rem = lon // LANES + 1, lon % LANES

    def write(row, pieces):
        folded = mirrored([jnp.concatenate([p(t) for p in pieces], axis=0) for t in range(tiles)], rem)
        folded[-1] = wrap_tile(folded[-1], folded[0], rem)
        for t in range(tiles):
            out[pl.ds(base + t * SMALL + row, 8), :] = folded[t]

    def current(c, row):
        return lambda t: -own_row(held, t, c, row)

    def column(row):
        return lambda t: held[pl.ds((t * 5 + 4) * 8 + row, 1), :]

    write(0, [current(0, 3), current(0, 2)])
    write(8, [current(1, 3), current(1, 2)])
    write(16, [current(1, 1)] + [column(3 - k) for k in range(4)])


def pack_kernel(offset, n, lon, small, *refs):
    if small:
        x_hbm, c_hbm, l_hbm, to_far, to_near, near_small, x, tail, sem, currents, levels, held, sems = refs
    else:
        x_hbm, to_far, to_near, x, tail, sem = refs
    full, rem = divmod(lon, LANES)
    size = (16 * full + 4) * n
    place = lax.axis_index("lat")
    top = place == lax.axis_size("lat") - 1
    copy = pltpu.make_async_copy(x_hbm.at[pl.ds(offset, n)], x, sem)
    if small:
        copies = [pltpu.make_async_copy(c_hbm, currents, sems.at[0]), pltpu.make_async_copy(l_hbm, levels, sems.at[1])]
        for c in copies:
            c.start()
        copy.start()
        odd = place % 2 == 1
        for c in copies:
            c.wait()
        stage_currents(currents, levels, held, lon)
        edge_rows(held, near_small, 0, jnp.logical_not(odd), lon)

        @pl.when(jnp.logical_not(top))
        def _():
            edge_rows(held, to_far, size, odd, lon)

        @pl.when(top)
        def _():
            folded_edge_rows(held, to_far, size, lon)
    else:
        copy.start()
    copy.wait()
    lane = lane_index()

    def joined(rests):
        out = rests[3]
        for r in range(3):
            out = jnp.where((lane >= r * rem) & (lane < (r + 1) * rem), rests[r], out)
        return out

    def pair(g, carry):
        first = pl.multiple_of(g * (32 * full), 8)
        for k in range(2):
            for level in range(4):
                for t in range(full):
                    tile = x[2 * g + k, level, :, pl.ds(t * LANES, LANES)]
                    to_near[pl.ds(first + t * 8 + 4 * k + level, 4, stride=full * 8), :] = tile
                rest = x[2 * g + k, level, :, pl.ds(full * LANES, rem)]
                tail[pl.ds(4 * k + level, 4, stride=8), :] = jnp.concatenate([rest] * (LANES // rem), axis=1)
        end = pl.multiple_of(16 * full * n + 8 * g, 8)
        to_near[pl.ds(end, 8), :] = joined([tail[pl.ds(8 * r, 8), :] for r in range(4)])

        @pl.when(jnp.logical_not(top))
        def _():
            for j in range(4 * full):
                to_far[pl.ds(first + j * 8, 8), :] = to_near[pl.ds(first + j * 8, 8), :]
            to_far[pl.ds(end, 8), :] = to_near[pl.ds(end, 8), :]

        @pl.when(top)
        def _():
            rests = []
            for r in range(4):
                source = 3 - r
                row = [to_near[pl.ds(first + (source * full + t) * 8, 8), :] for t in range(full)]
                row.append(tail[pl.ds(8 * source, 8), :])
                folded = mirrored(row, rem)
                for t in range(full):
                    to_far[pl.ds(first + (r * full + t) * 8, 8), :] = folded[t]
                rests.append(pltpu.roll(folded[full], r * rem, 1) if r else folded[full])
            to_far[pl.ds(end, 8), :] = joined(rests)

        return carry

    lax.fori_loop(0, n // 2, pair, 0)


def coefficient_kernel(n, lon, currents, levels, near, far, k1, k2, held, u, v, w):
    full, _ = divmod(lon, LANES)
    tiles = full + 1
    far_base = (16 * full + 4) * n
    place = lax.axis_index("lat")
    odd = place % 2 == 1
    level = (lax.broadcasted_iota(jnp.int32, (8, LANES), 0) % 4).astype(jnp.float32)
    stage_currents(currents, levels, held, lon)

    def put(dst, row, t, value):
        dst[pl.ds((row * tiles + t) * 8, 8), :] = value

    def get(src, row):
        return [src[pl.ds((row * tiles + t) * 8, 8), :] for t in range(tiles)]

    def twice(value):
        return jnp.concatenate([value, value], axis=0)

    for t in range(tiles):
        for row in range(4):
            put(u, 2 + row, t, twice(own_row(held, t, 0, row)))
            put(v, 3 + row, t, twice(own_row(held, t, 1, row)))
            column = spread(held, (t * 5 + 4) * 8 + row)
            put(w, 4 + row, t, (level < column).astype(jnp.float32))
        sides = ((0, 0, 0, True), (6, 7, 8, False))
        for u_row, v_row, w_row, is_low in sides:
            take_near = odd if is_low else jnp.logical_not(odd)

            def pick(start, size):
                a = near[pl.ds(t * SMALL + start, size), :]
                b = far[pl.ds(far_base + t * SMALL + start, size), :]
                return jnp.where(take_near, a, b)

            for k in range(2):
                put(u, u_row + k, t, twice(pick(4 * k, 4)))
            for k in range(3):
                put(v, v_row + k, t, twice(pick(8 + 4 * k, 4)))
            for k in range(4):
                put(w, w_row + k, t, (level < jnp.broadcast_to(pick(20 + k, 1), level.shape)).astype(jnp.float32))

    def parts(face):
        return jnp.maximum(face, 0.0) * (1.0 / 6.0), jnp.minimum(face, 0.0) * (1.0 / 6.0)

    def north_faces(row):
        wa, wb, va, vb = get(w, row + 4), get(w, row + 5), get(v, row + 3), get(v, row + 4)
        return [parts(wa[t] * wb[t] * (0.5 * (va[t] + vb[t]))) for t in range(tiles)]

    south = north_faces(-3)
    for row in range(-2, 6):
        north = north_faces(row)
        ur = get(u, row + 2)
        wr = {d: get(w, row + 4 + d) for d in (-2, -1, 0, 1, 2)}
        we = {d: [shifted(wr[0], t, d) for t in range(tiles)] for d in (-2, -1, 1, 2)}
        east = [parts(wr[0][t] * we[1][t] * (0.5 * (ur[t] + shifted(ur, t, 1)))) for t in range(tiles)]
        west_p = [shifted([e[0] for e in east], t, -1) for t in range(tiles)]
        west_m = [shifted([e[1] for e in east], t, -1) for t in range(tiles)]
        for t in range(tiles):
            (p, m), (q, s), (qs, ss) = east[t], north[t], south[t]
            pw, mw = west_p[t], west_m[t]
            plain = [
                -pw,
                p + 5.0 * pw + 2.0 * mw,
                -(2.0 * p + 5.0 * m + mw),
                m,
                1.0 - (5.0 * p + 2.0 * m) + (2.0 * pw + 5.0 * mw) - (5.0 * q + 2.0 * s) + (2.0 * qs + 5.0 * ss),
                -qs,
                q + 5.0 * qs + 2.0 * ss,
                -(2.0 * q + 5.0 * s + ss),
                s,
            ]
            source = [we[-2][t], we[-1][t], we[1][t], we[2][t], wr[0][t], wr[-2][t], wr[-1][t], wr[1][t], wr[2][t]]
            here = wr[0][t]
            half = 0.5 * here
            at1 = jnp.where(odd, row + 2, 5 - row) * (tiles * 9 * 8)
            at2 = jnp.where(odd, row, 3 - row) * (tiles * 10 * 8)
            for k in range(9):
                turn = k if k < 5 else jnp.where(odd, k, 13 - k)
                start = pl.multiple_of(at1 + (t * 9 + turn) * 8, 8)
                k1[pl.ds(start, 8), :] = plain[k] * source[k] * here
                if 0 <= row < 4:
                    start = pl.multiple_of(at2 + (t * 10 + turn) * 8, 8)
                    k2[pl.ds(start, 8), :] = plain[k] * half
            if 0 <= row < 4:
                start = pl.multiple_of(at2 + (t * 10 + 9) * 8, 8)
                k2[pl.ds(start, 8), :] = half * here
        south = north


def stencil(coefficients, here, before, after, rows):
    tiles = [here, after, before]
    values = [shifted(tiles, 0, d) for d in (-2, -1, 1, 2)] + [here] + rows
    total = coefficients[0] * values[0]
    for k in range(1, 9):
        total = total + coefficients[k] * values[k]
    return total


def advect_kernel(n, lon, groups, own, near, far, k1, k2, *refs):
    out, last, first, turned = refs[-4:]
    full, rem = divmod(lon, LANES)
    tiles = full + 1
    odd = lax.axis_index("lat") % 2 == 1
    group0 = pl.program_id(0) * groups
    physical = [jnp.where(odd, j, 3 - j) for j in range(4)]

    starts = [[pl.multiple_of((4 * (group0 + i) + physical[j]) * (full * 8), 8) for j in range(4)] for i in range(groups)]
    for i in range(groups):
        for side, source in enumerate((near, own, far)):
            rest = source[pl.ds(pl.multiple_of(16 * full * n + 8 * (group0 + i), 8), 8), :]
            for j in range(4):
                raw = pltpu.roll(rest, jnp.where(odd, (-j * rem) % LANES, ((j - 3) * rem) % LANES), 1)
                begin = source[pl.ds(starts[i][j], 8), :]
                last[pl.ds((i * 12 + side * 4 + j) * 8, 8), :] = wrap_tile(raw, begin, rem)

    def f(i, row, t):
        t = t % tiles
        side, j = divmod(row + 4, 4)
        if t == full:
            return last[pl.ds((i * 12 + side * 4 + j) * 8, 8), :]
        return (near, own, far)[side][pl.ds(starts[i][j] + t * 8, 8), :]

    def once(i, row, t):
        return ((i * 8 + row + 2) * tiles + t % tiles) * 8

    for t in range(tiles):
        column = [[f(i, row, t) for row in range(-4, 8)] for i in range(groups)]
        for row in range(-2, 6):
            base = ((row + 2) * tiles + t) * 9
            coefficients = [k1[pl.ds((base + k) * 8, 8), :] for k in range(9)]
            for i in range(groups):
                c = column[i]
                rows = [c[row + 4 + d] for d in (-2, -1, 1, 2)]
                value = stencil(coefficients, c[row + 4], f(i, row, t - 1), f(i, row, t + 1), rows)
                first[pl.ds(once(i, row, t), 8), :] = value

    for t in range(tiles):
        column = [[first[pl.ds(once(i, row, t), 8), :] for row in range(-2, 6)] for i in range(groups)]
        for row in range(4):
            base = (row * tiles + t) * 10
            coefficients = [k2[pl.ds((base + k) * 8, 8), :] for k in range(10)]
            for i in range(groups):
                c = column[i]
                rows = [c[row + 2 + d] for d in (-2, -1, 1, 2)]
                before, after = (first[pl.ds(once(i, row, t + d), 8), :] for d in (-1, 1))
                value = stencil(coefficients, c[row + 2], before, after, rows) + coefficients[9] * f(i, row, t)
                turned[pl.ds((i * tiles + t) * 32 + physical[row], 8, stride=4), :] = value
        for i in range(groups):
            for k in range(2):
                for level in range(4):
                    value = turned[pl.ds((i * tiles + t) * 32 + (4 * k + level) * 4, 4), :]
                    if t < full:
                        out[2 * i + k, level, :, pl.ds(t * LANES, LANES)] = value
                    else:
                        out[2 * i + k, level, :, pl.ds(full * LANES, rem)] = value[:, :rem]


def vmem():
    return pl.BlockSpec(memory_space=pltpu.VMEM)


def shards(tracers, currents, column_levels):
    count = lax.axis_size("lat")
    total, levels, rows, lon = tracers.shape
    full, rem = divmod(lon, LANES)
    tiles = full + 1
    assert levels == 4 and rows == 4 and 4 * rem == LANES and count % 2 == 0 and sum(CHUNKS) == total
    near_pairs = [(i, i ^ 1) for i in range(count)]
    far_pairs = [pair for i in range(1, count - 1, 2) for pair in ((i, i + 1), (i + 1, i))]
    far_pairs.append((count - 1, count - 1))
    f32 = jnp.float32

    packed, kept, near_small = [], [], None
    for i, (offset, n) in enumerate(zip(OFFSETS, CHUNKS)):
        small = i == 0
        size = (16 * full + 4) * n
        shape = [
            jax.ShapeDtypeStruct((size + (SMALL * tiles if small else 0), LANES), f32),
            jax.ShapeDtypeStruct((size, LANES), f32),
        ]
        scratch = [pltpu.VMEM((n, levels, rows, lon), f32), pltpu.VMEM((32, LANES), f32), pltpu.SemaphoreType.DMA]
        if small:
            shape.append(jax.ShapeDtypeStruct((SMALL * tiles, LANES), f32))
            scratch += [
                pltpu.VMEM(currents.shape, f32),
                pltpu.VMEM(column_levels.shape, jnp.int32),
                pltpu.VMEM((tiles * 40, LANES), f32),
                pltpu.SemaphoreType.DMA((2,)),
            ]
        result = pl.pallas_call(
            functools.partial(pack_kernel, offset, n, lon, small),
            out_shape=shape,
            in_specs=[pl.BlockSpec(memory_space=pltpu.HBM)] * (3 if small else 1),
            out_specs=[vmem() for _ in shape],
            scratch_shapes=scratch,
            cost_estimate=pl.CostEstimate(flops=1000000 * n, bytes_accessed=n * 184320, transcendentals=0),
            compiler_params=pltpu.CompilerParams(vmem_limit_bytes=16 * 2**20),
        )(tracers, *((currents, column_levels) if small else ()))
        packed.append(result[0])
        kept.append(result[1])
        if small:
            near_small = result[2]
    far = []
    for i in range(len(CHUNKS)):
        far.append(lax.ppermute(packed[i], "lat", far_pairs))
    small_received = lax.ppermute(near_small, "lat", near_pairs)
    near = []
    for i in range(len(CHUNKS)):
        near.append(lax.ppermute(kept[i], "lat", near_pairs))
    k1, k2 = pl.pallas_call(
        functools.partial(coefficient_kernel, CHUNKS[0], lon),
        out_shape=[
            jax.ShapeDtypeStruct((8 * tiles * 9 * 8, LANES), f32),
            jax.ShapeDtypeStruct((4 * tiles * 10 * 8, LANES), f32),
        ],
        in_specs=[vmem()] * 4,
        out_specs=[vmem()] * 2,
        scratch_shapes=[
            pltpu.VMEM((tiles * 40, LANES), f32),
            pltpu.VMEM((8 * tiles * 8, LANES), f32),
            pltpu.VMEM((10 * tiles * 8, LANES), f32),
            pltpu.VMEM((12 * tiles * 8, LANES), f32),
        ],
        cost_estimate=pl.CostEstimate(flops=8000000, bytes_accessed=6000000, transcendentals=0),
        compiler_params=pltpu.CompilerParams(vmem_limit_bytes=20 * 2**20),
        name="coefficients",
    )(currents, column_levels, small_received, far[0])
    out = None
    for i, (offset, n, groups) in enumerate(zip(OFFSETS, CHUNKS, GROUPS)):
        operands = [kept[i], near[i], far[i], k1, k2]
        specs = [vmem()] * 5
        aliases = {}
        if out is not None:
            aliases = {len(operands): 0}
            operands.append(out)
            specs.append(pl.BlockSpec(memory_space=pl.ANY))
        out = pl.pallas_call(
            functools.partial(advect_kernel, n, lon, groups),
            out_shape=jax.ShapeDtypeStruct(tracers.shape, f32),
            grid=(n // (2 * groups),),
            in_specs=specs,
            out_specs=pl.BlockSpec(
                (2 * groups, levels, rows, lon), lambda g, o=offset // (2 * groups): (o + g, 0, 0, 0)
            ),
            scratch_shapes=[
                pltpu.VMEM((groups * 12 * 8, LANES), f32),
                pltpu.VMEM((groups * 8 * tiles * 8, LANES), f32),
                pltpu.VMEM((groups * 32 * tiles, LANES), f32),
            ],
            input_output_aliases=aliases,
            cost_estimate=pl.CostEstimate(flops=3000000 * n, bytes_accessed=n * 500000, transcendentals=0),
            compiler_params=pltpu.CompilerParams(vmem_limit_bytes=24 * 2**20),
        )(*operands)
    return out


def solution(mesh):
    in_specs = (
        P("member", None, "lat", None),
        P("member", None, "lat", None),
        P(("member", "lat"), None),
    )
    out_specs = P("member", None, "lat", None)
    return jax.shard_map(shards, mesh=mesh, in_specs=in_specs, out_specs=out_specs, check_vma=False)
```

```python
import functools

import jax
import jax.numpy as jnp
from jax import lax
from jax.experimental import pallas as pl
from jax.experimental.pallas import tpu as pltpu
from jax.sharding import PartitionSpec as P


LANES = 128
SMALL = 24
CHUNKS = (12, 8, 6, 4)
OFFSETS = (0, 12, 24, 20)
GROUPS = (2, 2, 3, 2)


def lane_index():
    return lax.broadcasted_iota(jnp.int32, (8, LANES), 1)


def spread(ref, row):
    return jnp.broadcast_to(ref[pl.ds(row, 1), :], (8, LANES))


def wrap_tile(raw, first, rem):
    lane = lane_index()
    wrapped = jnp.where(
        lane < LANES - rem, pltpu.roll(first, rem, 1), pltpu.roll(raw, LANES - rem, 1)
    )
    return jnp.where(lane < rem, raw, wrapped)


def shifted(tiles, t, by):
    count = len(tiles)
    if by > 0:
        joined = jnp.where(lane_index() < by, tiles[(t + 1) % count], tiles[t])
    else:
        joined = jnp.where(lane_index() >= LANES + by, tiles[(t - 1) % count], tiles[t])
    return pltpu.roll(joined, (-by) % LANES, 1)


def mirrored(tiles, rem):
    lane = lane_index()
    index = (rem - 1 - lane) % LANES
    turned = [jnp.take_along_axis(tile, index, axis=1, mode="promise_in_bounds") for tile in tiles]
    last = len(tiles) - 1
    out = [jnp.where(lane < rem, turned[last - t], turned[last - 1 - t]) for t in range(last)]
    return [*out, turned[0]]


def natural_tile(ref, where, t, lon):
    full, rem = divmod(lon, LANES)
    if t < full:
        return ref[(*where, slice(None), pl.ds(t * LANES, LANES))]
    tail = ref[(*where, slice(None), pl.ds(full * LANES, rem))]
    head = ref[(*where, slice(None), pl.ds(0, LANES))][:, : LANES - 2 * rem]
    return jnp.concatenate([tail, head, tail], axis=1)


def stage_flow(flow, held, lon):
    for t in range(lon // LANES + 1):
        for part in range(4):
            pair = [natural_tile(flow, (2 * part + k,), t, lon) for k in range(2)]
            held[pl.ds((t * 5 + part) * 8, 8), :] = jnp.concatenate(pair, axis=0)
        column = natural_tile(flow, (8,), t, lon)
        held[pl.ds((t * 5 + 4) * 8, 8), :] = jnp.concatenate([column, column], axis=0)


def own_row(held, t, c, row):
    return held[pl.ds((t * 5 + 2 * c) * 8 + row, 4, stride=4), :]


def edge_rows(held, out, base, north, lon):
    u0, v0 = jnp.where(north, 2, 0), jnp.where(north, 1, 0)
    for t in range(lon // LANES + 1):
        u = [own_row(held, t, 0, u0 + k) for k in range(2)]
        v = [own_row(held, t, 1, v0 + k) for k in range(3)]
        column = held[pl.ds((t * 5 + 4) * 8, 4), :]
        start = base + t * SMALL
        out[pl.ds(start, 8), :] = jnp.concatenate(u, axis=0)
        out[pl.ds(start + 8, 8), :] = jnp.concatenate(v[:2], axis=0)
        out[pl.ds(start + 16, 8), :] = jnp.concatenate([v[2], column], axis=0)


def folded_edge_rows(held, out, base, lon):
    tiles, rem = lon // LANES + 1, lon % LANES

    def write(row, pieces):
        folded = mirrored([jnp.concatenate([p(t) for p in pieces], axis=0) for t in range(tiles)], rem)
        folded[-1] = wrap_tile(folded[-1], folded[0], rem)
        for t in range(tiles):
            out[pl.ds(base + t * SMALL + row, 8), :] = folded[t]

    def current(c, row):
        return lambda t: -own_row(held, t, c, row)

    def column(row):
        return lambda t: held[pl.ds((t * 5 + 4) * 8 + row, 1), :]

    write(0, [current(0, 3), current(0, 2)])
    write(8, [current(1, 3), current(1, 2)])
    write(16, [current(1, 1)] + [column(3 - k) for k in range(4)])


def pack_kernel(offset, n, lon, small, *refs):
    if small:
        x, flow, to_far, to_near, near_small, tail, held = refs
    else:
        x, to_far, to_near, tail = refs
    full, rem = divmod(lon, LANES)
    size = (16 * full + 4) * n
    place = lax.axis_index("lat")
    top = place == lax.axis_size("lat") - 1
    if small:
        odd = place % 2 == 1
        stage_flow(flow, held, lon)
        edge_rows(held, near_small, 0, jnp.logical_not(odd), lon)

        @pl.when(jnp.logical_not(top))
        def _():
            edge_rows(held, to_far, size, odd, lon)

        @pl.when(top)
        def _():
            folded_edge_rows(held, to_far, size, lon)

    lane = lane_index()

    def joined(rests):
        out = rests[3]
        for r in range(3):
            out = jnp.where((lane >= r * rem) & (lane < (r + 1) * rem), rests[r], out)
        return out

    def pair(g, carry):
        first = pl.multiple_of(g * (32 * full), 8)
        for k in range(2):
            for level in range(4):
                for t in range(full):
                    tile = x[offset + 2 * g + k, level, :, pl.ds(t * LANES, LANES)]
                    to_near[pl.ds(first + t * 8 + 4 * k + level, 4, stride=full * 8), :] = tile
                rest = x[offset + 2 * g + k, level, :, pl.ds(full * LANES, rem)]
                tail[pl.ds(4 * k + level, 4, stride=8), :] = jnp.concatenate([rest] * (LANES // rem), axis=1)
        end = pl.multiple_of(16 * full * n + 8 * g, 8)
        to_near[pl.ds(end, 8), :] = joined([tail[pl.ds(8 * r, 8), :] for r in range(4)])

        @pl.when(jnp.logical_not(top))
        def _():
            for j in range(4 * full):
                to_far[pl.ds(first + j * 8, 8), :] = to_near[pl.ds(first + j * 8, 8), :]
            to_far[pl.ds(end, 8), :] = to_near[pl.ds(end, 8), :]

        @pl.when(top)
        def _():
            rests = []
            for r in range(4):
                source = 3 - r
                row = [to_near[pl.ds(first + (source * full + t) * 8, 8), :] for t in range(full)]
                row.append(tail[pl.ds(8 * source, 8), :])
                folded = mirrored(row, rem)
                for t in range(full):
                    to_far[pl.ds(first + (r * full + t) * 8, 8), :] = folded[t]
                rests.append(pltpu.roll(folded[full], r * rem, 1) if r else folded[full])
            to_far[pl.ds(end, 8), :] = joined(rests)

        return carry

    lax.fori_loop(0, n // 2, pair, 0)


def coefficient_kernel(n, lon, flow, near, far, k1, k2, held, u, v, w):
    full, _ = divmod(lon, LANES)
    tiles = full + 1
    far_base = (16 * full + 4) * n
    place = lax.axis_index("lat")
    odd = place % 2 == 1
    level = (lax.broadcasted_iota(jnp.int32, (8, LANES), 0) % 4).astype(jnp.float32)
    stage_flow(flow, held, lon)

    def put(dst, row, t, value):
        dst[pl.ds((row * tiles + t) * 8, 8), :] = value

    def get(src, row):
        return [src[pl.ds((row * tiles + t) * 8, 8), :] for t in range(tiles)]

    def twice(value):
        return jnp.concatenate([value, value], axis=0)

    for t in range(tiles):
        for row in range(4):
            put(u, 2 + row, t, twice(own_row(held, t, 0, row)))
            put(v, 3 + row, t, twice(own_row(held, t, 1, row)))
            column = spread(held, (t * 5 + 4) * 8 + row)
            put(w, 4 + row, t, (level < column).astype(jnp.float32))
        sides = ((0, 0, 0, True), (6, 7, 8, False))
        for u_row, v_row, w_row, is_low in sides:
            take_near = odd if is_low else jnp.logical_not(odd)

            def pick(start, size):
                a = near[pl.ds(t * SMALL + start, size), :]
                b = far[pl.ds(far_base + t * SMALL + start, size), :]
                return jnp.where(take_near, a, b)

            for k in range(2):
                put(u, u_row + k, t, twice(pick(4 * k, 4)))
            for k in range(3):
                put(v, v_row + k, t, twice(pick(8 + 4 * k, 4)))
            for k in range(4):
                put(w, w_row + k, t, (level < jnp.broadcast_to(pick(20 + k, 1), level.shape)).astype(jnp.float32))

    def parts(face):
        return jnp.maximum(face, 0.0) * (1.0 / 6.0), jnp.minimum(face, 0.0) * (1.0 / 6.0)

    def north_faces(row):
        wa, wb, va, vb = get(w, row + 4), get(w, row + 5), get(v, row + 3), get(v, row + 4)
        return [parts(wa[t] * wb[t] * (0.5 * (va[t] + vb[t]))) for t in range(tiles)]

    south = north_faces(-3)
    for row in range(-2, 6):
        north = north_faces(row)
        ur = get(u, row + 2)
        wr = {d: get(w, row + 4 + d) for d in (-2, -1, 0, 1, 2)}
        we = {d: [shifted(wr[0], t, d) for t in range(tiles)] for d in (-2, -1, 1, 2)}
        east = [parts(wr[0][t] * we[1][t] * (0.5 * (ur[t] + shifted(ur, t, 1)))) for t in range(tiles)]
        west_p = [shifted([e[0] for e in east], t, -1) for t in range(tiles)]
        west_m = [shifted([e[1] for e in east], t, -1) for t in range(tiles)]
        for t in range(tiles):
            (p, m), (q, s), (qs, ss) = east[t], north[t], south[t]
            pw, mw = west_p[t], west_m[t]
            plain = [
                -pw,
                p + 5.0 * pw + 2.0 * mw,
                -(2.0 * p + 5.0 * m + mw),
                m,
                1.0 - (5.0 * p + 2.0 * m) + (2.0 * pw + 5.0 * mw) - (5.0 * q + 2.0 * s) + (2.0 * qs + 5.0 * ss),
                -qs,
                q + 5.0 * qs + 2.0 * ss,
                -(2.0 * q + 5.0 * s + ss),
                s,
            ]
            source = [we[-2][t], we[-1][t], we[1][t], we[2][t], wr[0][t], wr[-2][t], wr[-1][t], wr[1][t], wr[2][t]]
            here = wr[0][t]
            half = 0.5 * here
            at1 = jnp.where(odd, row + 2, 5 - row) * (tiles * 9 * 8)
            at2 = jnp.where(odd, row, 3 - row) * (tiles * 10 * 8)
            for k in range(9):
                turn = k if k < 5 else jnp.where(odd, k, 13 - k)
                start = pl.multiple_of(at1 + (t * 9 + turn) * 8, 8)
                k1[pl.ds(start, 8), :] = plain[k] * source[k] * here
                if 0 <= row < 4:
                    start = pl.multiple_of(at2 + (t * 10 + turn) * 8, 8)
                    k2[pl.ds(start, 8), :] = plain[k] * half
            if 0 <= row < 4:
                start = pl.multiple_of(at2 + (t * 10 + 9) * 8, 8)
                k2[pl.ds(start, 8), :] = half * here
        south = north


def stencil(coefficients, here, before, after, rows):
    tiles = [here, after, before]
    values = [shifted(tiles, 0, d) for d in (-2, -1, 1, 2)] + [here] + rows
    total = coefficients[0] * values[0]
    for k in range(1, 9):
        total = total + coefficients[k] * values[k]
    return total


def advect_kernel(n, lon, groups, own, near, far, k1, k2, *refs):
    out, last, first, turned = refs[-4:]
    full, rem = divmod(lon, LANES)
    tiles = full + 1
    odd = lax.axis_index("lat") % 2 == 1
    group0 = pl.program_id(0) * groups
    physical = [jnp.where(odd, j, 3 - j) for j in range(4)]

    starts = [[pl.multiple_of((4 * (group0 + i) + physical[j]) * (full * 8), 8) for j in range(4)] for i in range(groups)]
    for i in range(groups):
        for side, source in enumerate((near, own, far)):
            rest = source[pl.ds(pl.multiple_of(16 * full * n + 8 * (group0 + i), 8), 8), :]
            for j in range(4):
                raw = pltpu.roll(rest, jnp.where(odd, (-j * rem) % LANES, ((j - 3) * rem) % LANES), 1)
                begin = source[pl.ds(starts[i][j], 8), :]
                last[pl.ds((i * 12 + side * 4 + j) * 8, 8), :] = wrap_tile(raw, begin, rem)

    def f(i, row, t):
        t = t % tiles
        side, j = divmod(row + 4, 4)
        if t == full:
            return last[pl.ds((i * 12 + side * 4 + j) * 8, 8), :]
        return (near, own, far)[side][pl.ds(starts[i][j] + t * 8, 8), :]

    def once(i, row, t):
        return ((i * 8 + row + 2) * tiles + t % tiles) * 8

    for t in range(tiles):
        column = [[f(i, row, t) for row in range(-4, 8)] for i in range(groups)]
        for row in range(-2, 6):
            base = ((row + 2) * tiles + t) * 9
            coefficients = [k1[pl.ds((base + k) * 8, 8), :] for k in range(9)]
            for i in range(groups):
                c = column[i]
                rows = [c[row + 4 + d] for d in (-2, -1, 1, 2)]
                value = stencil(coefficients, c[row + 4], f(i, row, t - 1), f(i, row, t + 1), rows)
                first[pl.ds(once(i, row, t), 8), :] = value

    for t in range(tiles):
        column = [[first[pl.ds(once(i, row, t), 8), :] for row in range(-2, 6)] for i in range(groups)]
        for row in range(4):
            base = (row * tiles + t) * 10
            coefficients = [k2[pl.ds((base + k) * 8, 8), :] for k in range(10)]
            for i in range(groups):
                c = column[i]
                rows = [c[row + 2 + d] for d in (-2, -1, 1, 2)]
                before, after = (first[pl.ds(once(i, row, t + d), 8), :] for d in (-1, 1))
                value = stencil(coefficients, c[row + 2], before, after, rows) + coefficients[9] * f(i, row, t)
                turned[pl.ds((i * tiles + t) * 32 + physical[row], 8, stride=4), :] = value
        for i in range(groups):
            for k in range(2):
                for level in range(4):
                    value = turned[pl.ds((i * tiles + t) * 32 + (4 * k + level) * 4, 4), :]
                    if t < full:
                        out[2 * i + k, level, :, pl.ds(t * LANES, LANES)] = value
                    else:
                        out[2 * i + k, level, :, pl.ds(full * LANES, rem)] = value[:, :rem]


def vmem():
    return pl.BlockSpec(memory_space=pltpu.VMEM)


def shards(tracers, currents, column_levels):
    count = lax.axis_size("lat")
    total, levels, rows, lon = tracers.shape
    full, rem = divmod(lon, LANES)
    tiles = full + 1
    assert levels == 4 and rows == 4 and 4 * rem == LANES and count % 2 == 0 and sum(CHUNKS) == total
    near_pairs = [(i, i ^ 1) for i in range(count)]
    far_pairs = [pair for i in range(1, count - 1, 2) for pair in ((i, i + 1), (i + 1, i))]
    far_pairs.append((count - 1, count - 1))
    f32 = jnp.float32

    packed, kept, near_small = [], [], None
    merged = currents.reshape(2 * levels, rows, lon)
    flow = jnp.concatenate([merged, column_levels.astype(f32)[None]], axis=0)
    for i, (offset, n) in enumerate(zip(OFFSETS, CHUNKS)):
        small = i == 0
        size = (16 * full + 4) * n
        shape = [
            jax.ShapeDtypeStruct((size + (SMALL * tiles if small else 0), LANES), f32),
            jax.ShapeDtypeStruct((size, LANES), f32),
        ]
        scratch = [pltpu.VMEM((32, LANES), f32)]
        if small:
            shape.append(jax.ShapeDtypeStruct((SMALL * tiles, LANES), f32))
            scratch.append(pltpu.VMEM((tiles * 40, LANES), f32))
        result = pl.pallas_call(
            functools.partial(pack_kernel, offset, n, lon, small),
            out_shape=shape,
            in_specs=[vmem()] * (2 if small else 1),
            out_specs=[vmem() for _ in shape],
            scratch_shapes=scratch,
            cost_estimate=pl.CostEstimate(flops=1000000 * n, bytes_accessed=n * 184320, transcendentals=0),
            compiler_params=pltpu.CompilerParams(vmem_limit_bytes=16 * 2**20),
        )(tracers, *((flow,) if small else ()))
        packed.append(result[0])
        kept.append(result[1])
        if small:
            near_small = result[2]
    far = []
    for i in range(len(CHUNKS)):
        far.append(lax.ppermute(packed[i], "lat", far_pairs))
    small_received = lax.ppermute(near_small, "lat", near_pairs)
    near = []
    for i in range(len(CHUNKS)):
        near.append(lax.ppermute(kept[i], "lat", near_pairs))
    k1, k2 = pl.pallas_call(
        functools.partial(coefficient_kernel, CHUNKS[0], lon),
        out_shape=[
            jax.ShapeDtypeStruct((8 * tiles * 9 * 8, LANES), f32),
            jax.ShapeDtypeStruct((4 * tiles * 10 * 8, LANES), f32),
        ],
        in_specs=[vmem()] * 3,
        out_specs=[vmem()] * 2,
        scratch_shapes=[
            pltpu.VMEM((tiles * 40, LANES), f32),
            pltpu.VMEM((8 * tiles * 8, LANES), f32),
            pltpu.VMEM((10 * tiles * 8, LANES), f32),
            pltpu.VMEM((12 * tiles * 8, LANES), f32),
        ],
        cost_estimate=pl.CostEstimate(flops=8000000, bytes_accessed=6000000, transcendentals=0),
        compiler_params=pltpu.CompilerParams(vmem_limit_bytes=20 * 2**20),
        name="coefficients",
    )(flow, small_received, far[0])
    out = None
    for i, (offset, n, groups) in enumerate(zip(OFFSETS, CHUNKS, GROUPS)):
        operands = [kept[i], near[i], far[i], k1, k2]
        specs = [vmem()] * 5
        aliases = {}
        if out is not None:
            aliases = {len(operands): 0}
            operands.append(out)
            specs.append(pl.BlockSpec(memory_space=pl.ANY))
        out = pl.pallas_call(
            functools.partial(advect_kernel, n, lon, groups),
            out_shape=jax.ShapeDtypeStruct(tracers.shape, f32),
            grid=(n // (2 * groups),),
            in_specs=specs,
            out_specs=pl.BlockSpec(
                (2 * groups, levels, rows, lon), lambda g, o=offset // (2 * groups): (o + g, 0, 0, 0)
            ),
            scratch_shapes=[
                pltpu.VMEM((groups * 12 * 8, LANES), f32),
                pltpu.VMEM((groups * 8 * tiles * 8, LANES), f32),
                pltpu.VMEM((groups * 32 * tiles, LANES), f32),
            ],
            input_output_aliases=aliases,
            cost_estimate=pl.CostEstimate(flops=3000000 * n, bytes_accessed=n * 500000, transcendentals=0),
            compiler_params=pltpu.CompilerParams(vmem_limit_bytes=24 * 2**20),
        )(*operands)
    return out


def solution(mesh):
    in_specs = (
        P("member", None, "lat", None),
        P("member", None, "lat", None),
        P(("member", "lat"), None),
    )
    out_specs = P("member", None, "lat", None)
    return jax.shard_map(shards, mesh=mesh, in_specs=in_specs, out_specs=out_specs, check_vma=False)
```

```python
import functools

import jax
import jax.numpy as jnp
from jax import lax
from jax.experimental import pallas as pl
from jax.experimental.pallas import tpu as pltpu
from jax.sharding import PartitionSpec as P


LANES = 128
SMALL = 24
CHUNKS = (8, 12, 6, 4)
OFFSETS = (0, 8, 24, 20)
GROUPS = (2, 2, 3, 2)


def lane_index():
    return lax.broadcasted_iota(jnp.int32, (8, LANES), 1)


def spread(ref, row):
    return jnp.broadcast_to(ref[pl.ds(row, 1), :], (8, LANES))


def wrap_tile(raw, first, rem):
    lane = lane_index()
    wrapped = jnp.where(
        lane < LANES - rem, pltpu.roll(first, rem, 1), pltpu.roll(raw, LANES - rem, 1)
    )
    return jnp.where(lane < rem, raw, wrapped)


def shifted(tiles, t, by):
    count = len(tiles)
    if by > 0:
        joined = jnp.where(lane_index() < by, tiles[(t + 1) % count], tiles[t])
    else:
        joined = jnp.where(lane_index() >= LANES + by, tiles[(t - 1) % count], tiles[t])
    return pltpu.roll(joined, (-by) % LANES, 1)


def mirrored(tiles, rem):
    lane = lane_index()
    index = (rem - 1 - lane) % LANES
    turned = [jnp.take_along_axis(tile, index, axis=1, mode="promise_in_bounds") for tile in tiles]
    last = len(tiles) - 1
    out = [jnp.where(lane < rem, turned[last - t], turned[last - 1 - t]) for t in range(last)]
    return [*out, turned[0]]


def natural_tile(ref, where, t, lon):
    full, rem = divmod(lon, LANES)
    if t < full:
        return ref[(*where, slice(None), pl.ds(t * LANES, LANES))]
    tail = ref[(*where, slice(None), pl.ds(full * LANES, rem))]
    head = ref[(*where, slice(None), pl.ds(0, LANES))][:, : LANES - 2 * rem]
    return jnp.concatenate([tail, head, tail], axis=1)


def stage_flow(currents, levels, held, lon):
    for t in range(lon // LANES + 1):
        for part in range(4):
            pair = [natural_tile(currents, (part // 2, 2 * (part % 2) + k), t, lon) for k in range(2)]
            held[pl.ds((t * 5 + part) * 8, 8), :] = jnp.concatenate(pair, axis=0)
        column = natural_tile(levels, (), t, lon).astype(jnp.float32)
        held[pl.ds((t * 5 + 4) * 8, 8), :] = jnp.concatenate([column, column], axis=0)


def own_row(held, t, c, row):
    return held[pl.ds((t * 5 + 2 * c) * 8 + row, 4, stride=4), :]


def edge_rows(held, out, base, north, lon):
    u0, v0 = jnp.where(north, 2, 0), jnp.where(north, 1, 0)
    for t in range(lon // LANES + 1):
        u = [own_row(held, t, 0, u0 + k) for k in range(2)]
        v = [own_row(held, t, 1, v0 + k) for k in range(3)]
        column = held[pl.ds((t * 5 + 4) * 8, 4), :]
        start = base + t * SMALL
        out[pl.ds(start, 8), :] = jnp.concatenate(u, axis=0)
        out[pl.ds(start + 8, 8), :] = jnp.concatenate(v[:2], axis=0)
        out[pl.ds(start + 16, 8), :] = jnp.concatenate([v[2], column], axis=0)


def folded_edge_rows(held, out, base, lon):
    tiles, rem = lon // LANES + 1, lon % LANES

    def write(row, pieces):
        folded = mirrored([jnp.concatenate([p(t) for p in pieces], axis=0) for t in range(tiles)], rem)
        folded[-1] = wrap_tile(folded[-1], folded[0], rem)
        for t in range(tiles):
            out[pl.ds(base + t * SMALL + row, 8), :] = folded[t]

    def current(c, row):
        return lambda t: -own_row(held, t, c, row)

    def column(row):
        return lambda t: held[pl.ds((t * 5 + 4) * 8 + row, 1), :]

    write(0, [current(0, 3), current(0, 2)])
    write(8, [current(1, 3), current(1, 2)])
    write(16, [current(1, 1)] + [column(3 - k) for k in range(4)])


def pack_kernel(offset, n, lon, small, *refs):
    if small:
        x_hbm, c_hbm, l_hbm, to_far, to_near, near_small, tail, held, x, currents, column, sems = refs
        sources = ((x_hbm.at[pl.ds(offset, n)], x), (c_hbm, currents), (l_hbm, column))
        copies = [pltpu.make_async_copy(a, b, sems.at[i]) for i, (a, b) in enumerate(sources)]
        for copy in copies:
            copy.start()
        start = 0
    else:
        x, to_far, to_near, tail = refs
        start = offset
    full, rem = divmod(lon, LANES)
    size = (16 * full + 4) * n
    place = lax.axis_index("lat")
    top = place == lax.axis_size("lat") - 1
    if small:
        odd = place % 2 == 1
        copies[1].wait()
        copies[2].wait()
        stage_flow(currents, column, held, lon)
        edge_rows(held, near_small, 0, jnp.logical_not(odd), lon)

        @pl.when(jnp.logical_not(top))
        def _():
            edge_rows(held, to_far, size, odd, lon)

        @pl.when(top)
        def _():
            folded_edge_rows(held, to_far, size, lon)

        copies[0].wait()
    lane = lane_index()

    def joined(rests):
        out = rests[3]
        for r in range(3):
            out = jnp.where((lane >= r * rem) & (lane < (r + 1) * rem), rests[r], out)
        return out

    def pair(g, carry):
        first = pl.multiple_of(g * (32 * full), 8)
        for k in range(2):
            for level in range(4):
                for t in range(full):
                    tile = x[start + 2 * g + k, level, :, pl.ds(t * LANES, LANES)]
                    to_near[pl.ds(first + t * 8 + 4 * k + level, 4, stride=full * 8), :] = tile
                rest = x[start + 2 * g + k, level, :, pl.ds(full * LANES, rem)]
                tail[pl.ds(4 * k + level, 4, stride=8), :] = jnp.concatenate([rest] * (LANES // rem), axis=1)
        end = pl.multiple_of(16 * full * n + 8 * g, 8)
        to_near[pl.ds(end, 8), :] = joined([tail[pl.ds(8 * r, 8), :] for r in range(4)])

        @pl.when(jnp.logical_not(top))
        def _():
            for j in range(4 * full):
                to_far[pl.ds(first + j * 8, 8), :] = to_near[pl.ds(first + j * 8, 8), :]
            to_far[pl.ds(end, 8), :] = to_near[pl.ds(end, 8), :]

        @pl.when(top)
        def _():
            rests = []
            for r in range(4):
                source = 3 - r
                row = [to_near[pl.ds(first + (source * full + t) * 8, 8), :] for t in range(full)]
                row.append(tail[pl.ds(8 * source, 8), :])
                folded = mirrored(row, rem)
                for t in range(full):
                    to_far[pl.ds(first + (r * full + t) * 8, 8), :] = folded[t]
                rests.append(pltpu.roll(folded[full], r * rem, 1) if r else folded[full])
            to_far[pl.ds(end, 8), :] = joined(rests)

        return carry

    lax.fori_loop(0, n // 2, pair, 0)


def coefficient_kernel(n, lon, currents, levels, near, far, k1, k2, held, u, v, w):
    full, _ = divmod(lon, LANES)
    tiles = full + 1
    far_base = (16 * full + 4) * n
    place = lax.axis_index("lat")
    odd = place % 2 == 1
    level = (lax.broadcasted_iota(jnp.int32, (8, LANES), 0) % 4).astype(jnp.float32)
    stage_flow(currents, levels, held, lon)

    def put(dst, row, t, value):
        dst[pl.ds((row * tiles + t) * 8, 8), :] = value

    def get(src, row):
        return [src[pl.ds((row * tiles + t) * 8, 8), :] for t in range(tiles)]

    def twice(value):
        return jnp.concatenate([value, value], axis=0)

    for t in range(tiles):
        for row in range(4):
            put(u, 2 + row, t, twice(own_row(held, t, 0, row)))
            put(v, 3 + row, t, twice(own_row(held, t, 1, row)))
            column = spread(held, (t * 5 + 4) * 8 + row)
            put(w, 4 + row, t, (level < column).astype(jnp.float32))
        sides = ((0, 0, 0, True), (6, 7, 8, False))
        for u_row, v_row, w_row, is_low in sides:
            take_near = odd if is_low else jnp.logical_not(odd)

            def pick(start, size):
                a = near[pl.ds(t * SMALL + start, size), :]
                b = far[pl.ds(far_base + t * SMALL + start, size), :]
                return jnp.where(take_near, a, b)

            for k in range(2):
                put(u, u_row + k, t, twice(pick(4 * k, 4)))
            for k in range(3):
                put(v, v_row + k, t, twice(pick(8 + 4 * k, 4)))
            for k in range(4):
                put(w, w_row + k, t, (level < jnp.broadcast_to(pick(20 + k, 1), level.shape)).astype(jnp.float32))

    def parts(face):
        return jnp.maximum(face, 0.0) * (1.0 / 6.0), jnp.minimum(face, 0.0) * (1.0 / 6.0)

    def north_faces(row):
        wa, wb, va, vb = get(w, row + 4), get(w, row + 5), get(v, row + 3), get(v, row + 4)
        return [parts(wa[t] * wb[t] * (0.5 * (va[t] + vb[t]))) for t in range(tiles)]

    south = north_faces(-3)
    for row in range(-2, 6):
        north = north_faces(row)
        ur = get(u, row + 2)
        wr = {d: get(w, row + 4 + d) for d in (-2, -1, 0, 1, 2)}
        we = {d: [shifted(wr[0], t, d) for t in range(tiles)] for d in (-2, -1, 1, 2)}
        east = [parts(wr[0][t] * we[1][t] * (0.5 * (ur[t] + shifted(ur, t, 1)))) for t in range(tiles)]
        west_p = [shifted([e[0] for e in east], t, -1) for t in range(tiles)]
        west_m = [shifted([e[1] for e in east], t, -1) for t in range(tiles)]
        for t in range(tiles):
            (p, m), (q, s), (qs, ss) = east[t], north[t], south[t]
            pw, mw = west_p[t], west_m[t]
            plain = [
                -pw,
                p + 5.0 * pw + 2.0 * mw,
                -(2.0 * p + 5.0 * m + mw),
                m,
                1.0 - (5.0 * p + 2.0 * m) + (2.0 * pw + 5.0 * mw) - (5.0 * q + 2.0 * s) + (2.0 * qs + 5.0 * ss),
                -qs,
                q + 5.0 * qs + 2.0 * ss,
                -(2.0 * q + 5.0 * s + ss),
                s,
            ]
            source = [we[-2][t], we[-1][t], we[1][t], we[2][t], wr[0][t], wr[-2][t], wr[-1][t], wr[1][t], wr[2][t]]
            here = wr[0][t]
            half = 0.5 * here
            at1 = jnp.where(odd, row + 2, 5 - row) * (tiles * 9 * 8)
            at2 = jnp.where(odd, row, 3 - row) * (tiles * 10 * 8)
            for k in range(9):
                turn = k if k < 5 else jnp.where(odd, k, 13 - k)
                start = pl.multiple_of(at1 + (t * 9 + turn) * 8, 8)
                k1[pl.ds(start, 8), :] = plain[k] * source[k] * here
                if 0 <= row < 4:
                    start = pl.multiple_of(at2 + (t * 10 + turn) * 8, 8)
                    k2[pl.ds(start, 8), :] = plain[k] * half
            if 0 <= row < 4:
                start = pl.multiple_of(at2 + (t * 10 + 9) * 8, 8)
                k2[pl.ds(start, 8), :] = half * here
        south = north


def stencil(coefficients, here, before, after, rows):
    tiles = [here, after, before]
    values = [shifted(tiles, 0, d) for d in (-2, -1, 1, 2)] + [here] + rows
    total = coefficients[0] * values[0]
    for k in range(1, 9):
        total = total + coefficients[k] * values[k]
    return total


def advect_kernel(n, lon, groups, own, near, far, k1, k2, *refs):
    out, last, first, turned = refs[-4:]
    full, rem = divmod(lon, LANES)
    tiles = full + 1
    odd = lax.axis_index("lat") % 2 == 1
    group0 = pl.program_id(0) * groups
    physical = [jnp.where(odd, j, 3 - j) for j in range(4)]

    starts = [[pl.multiple_of((4 * (group0 + i) + physical[j]) * (full * 8), 8) for j in range(4)] for i in range(groups)]
    for i in range(groups):
        for side, source in enumerate((near, own, far)):
            rest = source[pl.ds(pl.multiple_of(16 * full * n + 8 * (group0 + i), 8), 8), :]
            for j in range(4):
                raw = pltpu.roll(rest, jnp.where(odd, (-j * rem) % LANES, ((j - 3) * rem) % LANES), 1)
                begin = source[pl.ds(starts[i][j], 8), :]
                last[pl.ds((i * 12 + side * 4 + j) * 8, 8), :] = wrap_tile(raw, begin, rem)

    def f(i, row, t):
        t = t % tiles
        side, j = divmod(row + 4, 4)
        if t == full:
            return last[pl.ds((i * 12 + side * 4 + j) * 8, 8), :]
        return (near, own, far)[side][pl.ds(starts[i][j] + t * 8, 8), :]

    def once(i, row, t):
        return ((i * 8 + row + 2) * tiles + t % tiles) * 8

    for t in range(tiles):
        column = [[f(i, row, t) for row in range(-4, 8)] for i in range(groups)]
        for row in range(-2, 6):
            base = ((row + 2) * tiles + t) * 9
            coefficients = [k1[pl.ds((base + k) * 8, 8), :] for k in range(9)]
            for i in range(groups):
                c = column[i]
                rows = [c[row + 4 + d] for d in (-2, -1, 1, 2)]
                value = stencil(coefficients, c[row + 4], f(i, row, t - 1), f(i, row, t + 1), rows)
                first[pl.ds(once(i, row, t), 8), :] = value

    for t in range(tiles):
        column = [[first[pl.ds(once(i, row, t), 8), :] for row in range(-2, 6)] for i in range(groups)]
        for row in range(4):
            base = (row * tiles + t) * 10
            coefficients = [k2[pl.ds((base + k) * 8, 8), :] for k in range(10)]
            for i in range(groups):
                c = column[i]
                rows = [c[row + 2 + d] for d in (-2, -1, 1, 2)]
                before, after = (first[pl.ds(once(i, row, t + d), 8), :] for d in (-1, 1))
                value = stencil(coefficients, c[row + 2], before, after, rows) + coefficients[9] * f(i, row, t)
                turned[pl.ds((i * tiles + t) * 32 + physical[row], 8, stride=4), :] = value
        for i in range(groups):
            for k in range(2):
                for level in range(4):
                    value = turned[pl.ds((i * tiles + t) * 32 + (4 * k + level) * 4, 4), :]
                    if t < full:
                        out[2 * i + k, level, :, pl.ds(t * LANES, LANES)] = value
                    else:
                        out[2 * i + k, level, :, pl.ds(full * LANES, rem)] = value[:, :rem]


def vmem():
    return pl.BlockSpec(memory_space=pltpu.VMEM)


def shards(tracers, currents, column_levels):
    count = lax.axis_size("lat")
    total, levels, rows, lon = tracers.shape
    full, rem = divmod(lon, LANES)
    tiles = full + 1
    assert levels == 4 and rows == 4 and 4 * rem == LANES and count % 2 == 0 and sum(CHUNKS) == total
    near_pairs = [(i, i ^ 1) for i in range(count)]
    far_pairs = [pair for i in range(1, count - 1, 2) for pair in ((i, i + 1), (i + 1, i))]
    far_pairs.append((count - 1, count - 1))
    f32 = jnp.float32

    packed, kept, near_small = [], [], None
    for i, (offset, n) in enumerate(zip(OFFSETS, CHUNKS)):
        small = i == 0
        size = (16 * full + 4) * n
        shape = [
            pltpu.VMEM((size + (SMALL * tiles if small else 0), LANES), f32),
            pltpu.VMEM((size, LANES), f32),
        ]
        scratch = [pltpu.VMEM((32, LANES), f32)]
        if small:
            shape.append(pltpu.VMEM((SMALL * tiles, LANES), f32))
            scratch += [
                pltpu.VMEM((tiles * 40, LANES), f32),
                pltpu.VMEM((n, levels, rows, lon), f32),
                pltpu.VMEM(currents.shape, f32),
                pltpu.VMEM(column_levels.shape, jnp.int32),
                pltpu.SemaphoreType.DMA((3,)),
            ]
        result = pl.pallas_call(
            functools.partial(pack_kernel, offset, n, lon, small),
            out_shape=shape,
            in_specs=[pl.BlockSpec(memory_space=pltpu.HBM)] * 3 if small else [vmem()],
            out_specs=[vmem() for _ in shape],
            scratch_shapes=scratch,
            cost_estimate=pl.CostEstimate(flops=1000000 * n, bytes_accessed=n * 184320, transcendentals=0),
            compiler_params=pltpu.CompilerParams(vmem_limit_bytes=(56 if small else 16) * 2**20),
        )(tracers, *((currents, column_levels) if small else ()))
        packed.append(result[0])
        kept.append(result[1])
        if small:
            near_small = result[2]
    far = []
    for i in range(len(CHUNKS)):
        far.append(lax.ppermute(packed[i], "lat", far_pairs))
    small_received = lax.ppermute(near_small, "lat", near_pairs)
    near = []
    for i in range(len(CHUNKS)):
        near.append(lax.ppermute(kept[i], "lat", near_pairs))
    k1, k2 = pl.pallas_call(
        functools.partial(coefficient_kernel, CHUNKS[0], lon),
        out_shape=[
            jax.ShapeDtypeStruct((8 * tiles * 9 * 8, LANES), f32),
            jax.ShapeDtypeStruct((4 * tiles * 10 * 8, LANES), f32),
        ],
        in_specs=[vmem()] * 4,
        out_specs=[vmem()] * 2,
        scratch_shapes=[
            pltpu.VMEM((tiles * 40, LANES), f32),
            pltpu.VMEM((8 * tiles * 8, LANES), f32),
            pltpu.VMEM((10 * tiles * 8, LANES), f32),
            pltpu.VMEM((12 * tiles * 8, LANES), f32),
        ],
        cost_estimate=pl.CostEstimate(flops=8000000, bytes_accessed=6000000, transcendentals=0),
        compiler_params=pltpu.CompilerParams(vmem_limit_bytes=20 * 2**20),
        name="coefficients",
    )(currents, column_levels, small_received, far[0])
    out = None
    for i, (offset, n, groups) in enumerate(zip(OFFSETS, CHUNKS, GROUPS)):
        operands = [kept[i], near[i], far[i], k1, k2]
        specs = [vmem()] * 5
        aliases = {}
        if out is not None:
            aliases = {len(operands): 0}
            operands.append(out)
            specs.append(pl.BlockSpec(memory_space=pl.ANY))
        out = pl.pallas_call(
            functools.partial(advect_kernel, n, lon, groups),
            out_shape=jax.ShapeDtypeStruct(tracers.shape, f32),
            grid=(n // (2 * groups),),
            in_specs=specs,
            out_specs=pl.BlockSpec(
                (2 * groups, levels, rows, lon), lambda g, o=offset // (2 * groups): (o + g, 0, 0, 0)
            ),
            scratch_shapes=[
                pltpu.VMEM((groups * 12 * 8, LANES), f32),
                pltpu.VMEM((groups * 8 * tiles * 8, LANES), f32),
                pltpu.VMEM((groups * 32 * tiles, LANES), f32),
            ],
            input_output_aliases=aliases,
            cost_estimate=pl.CostEstimate(flops=3000000 * n, bytes_accessed=n * 500000, transcendentals=0),
            compiler_params=pltpu.CompilerParams(vmem_limit_bytes=24 * 2**20),
        )(*operands)
    return out


def solution(mesh):
    in_specs = (
        P("member", None, "lat", None),
        P("member", None, "lat", None),
        P(("member", "lat"), None),
    )
    out_specs = P("member", None, "lat", None)
    return jax.shard_map(shards, mesh=mesh, in_specs=in_specs, out_specs=out_specs, check_vma=False)
```
